32 devices in a mesh: lon: 4 (over z), lat: 2 (over y), lev: 4 (over x, core).
Axes of the slice: x: 2, y: 2, z: 4, core: 2. Of those that a mesh axis runs over, the one named last changes fastest.
Arguments:
- fields: bfloat16 [8, 12, 48, 192], P('lev', 'lat', 'lon'), may hold values from -7 to 7
- w_qkv: bfloat16 [4, 192, 576], replicated, may hold values from -7 to 7
- w_out: bfloat16 [4, 192, 192], replicated, may hold values from -0.4375 to 0.4375
- w_up: bfloat16 [4, 192, 768], replicated, may hold values from -0.4375 to 0.4375
- w_down: bfloat16 [4, 768, 192], replicated, may hold values from -0.21875 to 0.21875
- gains: float32 [4, 2, 192], replicated, may hold values from 0.25 to 1.75
- bias_table: bfloat16 [4, 4, 2, 6, 3312], P(None, None, 'lat'), may hold values from -4 to 4
- labels: int32 [8, 12, 48], P(None, 'lat', 'lon'), may hold values from 0 to 7, as said below
Outputs:
- fields_out: bfloat16 [8, 12, 48, 192], P('lev', 'lat', 'lon')
The draws below stay inside these ranges and needn't reach their ends.
Inputs may be any that keep to these rules, and one draw needn't show every extreme that they name: labels[z, y, x] = e + 2 f + 4 g, the same for every x, where e is 1 when z >= 7, f is 1 when y >= 9, and g is 1 when the row (y + 3) mod 12 is one of the first n or the last s padding rows of the grid, with n and s between 1 and 3.
All inputs are finite; a program needn't handle non-finite values.
Results may differ from the reference program's by a relative error of at most 0.025.
Values may be sent and summed in bfloat16 or wider, within the bound.
A program may use at most 64 MiB of HBM per device.

```python
import jax
import jax.numpy as jnp
from jax import lax

D = 192
HEADS = 6
FF = 768
WZ = 2
WY = 6
WX = 12
BLOCKS = 4
HD = 32
LEVW = 4
Z = 8
LATW = 2
LONW = 4
LAT = 12
LON = 48
POS = 3312


def draw_fields(key, part):
    values = jnp.clip(jax.random.normal(key, (Z, LAT, LON, D), jnp.float32), -6.0, 6.0)
    return values.astype(jnp.bfloat16)


def draw_w_qkv(key, part):
    base_key = jax.random.fold_in(key, 0)
    limit_value = 6.0 * D ** (-0.5)
    weights = jnp.clip(jax.random.normal(base_key, (BLOCKS, D, 3 * D), jnp.float32) * D ** (-0.5), -limit_value, limit_value)
    return weights.astype(jnp.bfloat16)


def draw_labels(key, part):
    pad_counts = jax.random.randint(jax.random.fold_in(key, 17), (2,), 1, WY // 2 + 1, dtype=jnp.int32)
    frame_levels = jnp.arange(Z, dtype=jnp.int32)
    frame_rows = jnp.arange(LAT, dtype=jnp.int32)
    level_wrap = (frame_levels >= Z - WZ // 2).astype(jnp.int32)
    row_wrap = (frame_rows >= LAT - WY // 2).astype(jnp.int32)
    grid_rows = (frame_rows + WY // 2) % LAT
    padding = ((grid_rows < pad_counts[0]) | (grid_rows >= LAT - pad_counts[1])).astype(jnp.int32)
    plane = 2 * row_wrap + 4 * padding
    region = level_wrap[:, None] + plane[None, :]
    return jnp.broadcast_to(region[:, :, None], (Z, LAT, LON)).astype(jnp.int32)


def steps_of(own_key, extent, cuts, smallest, top_value):
    loudness = 1.0
    for axis_at, parts in cuts:
        draws = jax.random.uniform(jax.random.fold_in(jax.random.fold_in(own_key, 6), axis_at), (parts,), jnp.float32, smallest / len(cuts), top_value / len(cuts))
        loudness = loudness * jnp.repeat(jnp.exp(draws), extent[axis_at] // parts).reshape((-1,) + (1,) * (len(extent) - 1 - axis_at))
    return loudness


def noise(stream_key, extent, scale, limit, shards=(), held_as=jnp.bfloat16):
    values = jax.random.normal(stream_key, extent, jnp.float32) * scale
    if len(shards) > 0:
        values = steps_of(stream_key, extent, shards, -0.22, 0.18) * values
    return jnp.clip(values, min=-limit, max=limit).astype(held_as)


def setup_inputs(seed: int = 0) -> dict:
    key_list = jax.random.split(jax.random.key(seed), 9)
    fields = draw_fields(jax.random.fold_in(key_list[8], 71), 0)
    w_qkv = draw_w_qkv(jax.random.fold_in(key_list[8], 71), 0)
    w_out = noise(key_list[2], (BLOCKS, D, D), D ** -0.5, 0.4375)
    w_up = noise(key_list[3], (BLOCKS, D, FF), D ** -0.5, 0.4375)
    w_down = noise(key_list[4], (BLOCKS, FF, D), FF ** -0.5, 0.21875)
    gains = jnp.clip(1.0 + 0.15 * jax.random.normal(key_list[5], (BLOCKS, 2, D), jnp.float32), 0.25, 1.75)
    bias_table = noise(key_list[6], (BLOCKS, LEVW, LATW, HEADS, POS), 1.0, 4.0, ((2, 2),))
    labels = draw_labels(jax.random.fold_in(key_list[8], 71), 0)
    return dict(fields=fields, w_qkv=w_qkv, w_out=w_out, w_up=w_up, w_down=w_down, gains=gains, bias_table=bias_table, labels=labels)


def layer_norm(values, gain_row):
    floats = values.astype(jnp.float32)
    center = floats - lax.optimization_barrier(jnp.mean(floats, axis=-1, keepdims=True))
    spread = lax.optimization_barrier(jnp.mean(center * center, axis=-1, keepdims=True))
    return center * lax.rsqrt(spread + 1e-05) * gain_row.astype(jnp.float32)

def expand_bias(bias_rows):
    row_count = bias_rows.shape[0]
    shaped = bias_rows.astype(jnp.float32).reshape(row_count, HEADS, WZ, WZ, WY, WY, 2 * WX - 1)
    offset = jnp.arange(WX, dtype=jnp.int32)[:, None] - jnp.arange(WX, dtype=jnp.int32)[None, :] + (WX - 1)
    selector = (offset[:, :, None] == jnp.arange(2 * WX - 1, dtype=jnp.int32)[None, None, :]).astype(jnp.float32)
    spread_out = jnp.einsum('nhpqrsd,abd->nhpraqsb', shaped, selector, precision=lax.Precision.HIGHEST)
    size_window = WZ * WY * WX
    return spread_out.reshape(row_count, HEADS, size_window, size_window)

def attend(queries, key_part, val_part, bias_full, query_labels, key_labels):
    scores = jnp.einsum('wahd,wbhd->whab', queries.astype(jnp.float32), key_part.astype(jnp.float32))
    scores = scores * HD ** (-0.5)
    groups = bias_full.shape[0]
    scores = (scores.reshape((groups, -1) + scores.shape[1:]) + bias_full[:, None]).reshape(scores.shape)
    if query_labels is None:
        allowed = jnp.ones(scores.shape, dtype=bool)
    else:
        allowed = query_labels[:, None, :, None] == key_labels[:, None, None, :]
    masked = jnp.where(allowed, scores, -1e+30)
    row_max = lax.optimization_barrier(jnp.max(masked, axis=-1, keepdims=True))
    exp_terms = jnp.where(allowed, jnp.exp(masked - row_max), 0.0)
    weights = (exp_terms / lax.optimization_barrier(jnp.sum(exp_terms, axis=-1, keepdims=True))).astype(jnp.bfloat16)
    mixed_heads = jnp.einsum('whab,wbhd->wahd', weights.astype(jnp.float32), val_part.astype(jnp.float32))
    return mixed_heads.astype(jnp.bfloat16)

def attention_layer(frame_grid, qkv_weight, out_weight, bias_rows, labels, use_labels):
    level_windows = Z // WZ
    size_window = WZ * WY * WX
    proj_qkv = jnp.dot(frame_grid.reshape(-1, D), qkv_weight, preferred_element_type=jnp.float32).astype(jnp.bfloat16)
    arranged = proj_qkv.reshape(level_windows, WZ, LATW, WY, LONW, WX, 3 * D).transpose(2, 0, 4, 1, 3, 5, 6)
    arranged = arranged.reshape(LATW, level_windows * LONW, size_window, 3 * D)
    label_grid = labels.reshape(level_windows, WZ, LATW, WY, LONW, WX).transpose(2, 0, 4, 1, 3, 5)
    label_grid = label_grid.reshape(LATW, level_windows * LONW, size_window)
    row_tables = bias_rows.transpose(1, 0, 2, 3)

    def one_row(inputs):
        row_qkv, row_table, row_labels = inputs
        bias_full = expand_bias(row_table)
        queries = row_qkv[:, :, :D].reshape(-1, size_window, HEADS, HD)
        key_part = row_qkv[:, :, D:2 * D].reshape(-1, size_window, HEADS, HD)
        val_part = row_qkv[:, :, 2 * D:].reshape(-1, size_window, HEADS, HD)
        if use_labels:
            mixed_heads = attend(queries, key_part, val_part, bias_full, row_labels, row_labels)
        else:
            mixed_heads = attend(queries, key_part, val_part, bias_full, None, None)
        return mixed_heads.reshape(-1, size_window, D)
    window_out = lax.map(one_row, (arranged, row_tables, label_grid))
    grid_rows = window_out.reshape(LATW, level_windows, LONW, WZ, WY, WX, D).transpose(1, 3, 0, 4, 2, 5, 6).reshape(-1, D)
    projected = jnp.dot(grid_rows, out_weight, preferred_element_type=jnp.float32).astype(jnp.bfloat16)
    return projected.reshape(Z, LAT, LON, D)

def reference(fields, w_qkv, w_out, w_up, w_down, gains, bias_table, labels):
    stream = fields
    half_shift = (WZ // 2, WY // 2, WX // 2)
    for block_idx in range(BLOCKS):
        shifted = block_idx % 2 == 1
        normed = layer_norm(stream, gains[block_idx, 0]).astype(jnp.bfloat16)
        frame_grid = normed
        if shifted:
            frame_grid = jnp.roll(normed, (-half_shift[0], -half_shift[1], -half_shift[2]), axis=(0, 1, 2))
        attended = attention_layer(frame_grid, w_qkv[block_idx], w_out[block_idx], bias_table[block_idx], labels, shifted)
        if shifted:
            attended = jnp.roll(attended, half_shift, axis=(0, 1, 2))
        middle = (stream.astype(jnp.float32) + attended.astype(jnp.float32)).astype(jnp.bfloat16)
        normed_two = layer_norm(middle, gains[block_idx, 1]).astype(jnp.bfloat16)
        hidden = jax.nn.gelu(jnp.dot(normed_two.reshape(-1, D), w_up[block_idx], preferred_element_type=jnp.float32), approximate=False).astype(jnp.bfloat16)
        down_rows = jnp.dot(hidden, w_down[block_idx], preferred_element_type=jnp.float32).reshape(Z, LAT, LON, D)
        stream = (middle.astype(jnp.float32) + down_rows).astype(jnp.bfloat16)
    return stream
```

```python
import functools

import jax
import jax.numpy as jnp
import numpy as np
from jax import lax
from jax.experimental import pallas as pl
from jax.experimental.pallas import tpu as pltpu
from jax.sharding import PartitionSpec as P

HEADS = 6
WZ = 2
WY = 6
WX = 12
BLOCKS = 4
OCT = 8
XH = WX // 2
YH = WY // 2
OROWS = XH * 4
T = OCT * OROWS
G = WZ * 8
SPAN = 2 * WX - 1
TABW = 384
NEG = -1e30
MESH = pl.DeviceIdType.MESH
AXES = ("lon", "lev", "lat")


def bits(octant):
    return ((octant >> 2) & 1, (octant >> 1) & 1, octant & 1)


def token_maps():
    place_in = np.zeros((T, WZ * WY * 16), np.float32)
    lanes = np.zeros((T, T), np.float32)
    for row in range(T):
        octant, inner = divmod(row, OROWS)
        c, a, b = bits(octant)
        xl, yl = divmod(inner, 4)
        x = c * XH + xl
        lanes[x * G + a * 8 + b * 4 + yl, row] = 1.0
        if yl < YH:
            place_in[row, (a * WY + b * YH + yl) * 16 + x] = 1.0
    spread = np.zeros((WZ, WY * SPAN, TABW), np.float32)
    for zq in range(WZ):
        for yq in range(WY):
            for d in range(SPAN):
                lane = (SPAN - 1 - d) * G + zq * 8 + (yq // YH) * 4 + yq % YH
                spread[zq, yq * SPAN + d, lane] = 1.0
    return place_in, lanes, spread


def kernel(
    fields_ref, table_ref, labels_ref, gains_ref,
    place_hbm, back_hbm, lanes_hbm, spread_hbm, wq_hbm, wo_hbm, wu_hbm, wd_hbm,
    out_ref,
    place_ref, back_ref, lanes_ref, spread_ref,
    wq, wo, wu, wd, grid_buf, tabr, toep, bias, send_buf, recv_buf,
    c_sem, w_sem, send_sem, recv_sem,
):
    where = {axis: lax.axis_index(axis) for axis in AXES}
    count = {axis: lax.axis_size(axis) for axis in AXES}

    def device(offsets):
        return {
            axis: lax.rem(where[axis] + (off + count[axis]), count[axis])
            for axis, off in zip(AXES, offsets)
        }

    constant_copies = []
    constants = ((place_hbm, place_ref), (spread_hbm, spread_ref), (lanes_hbm, lanes_ref), (back_hbm, back_ref))
    for i, (src, dst) in enumerate(constants):
        copy = pltpu.make_async_copy(src, dst, c_sem.at[i])
        copy.start()
        constant_copies.append(copy)
    weight_copies = []
    for b in range(BLOCKS):
        for i, (src, dst) in enumerate(((wq_hbm, wq), (wo_hbm, wo), (wu_hbm, wu), (wd_hbm, wd))):
            copy = pltpu.make_async_copy(src.at[b], dst.at[b], w_sem.at[b, i])
            copy.start()
            weight_copies.append(copy)

    barrier = pltpu.get_barrier_semaphore()
    for octant in range(1, OCT):
        for sign in (1, -1):
            pl.semaphore_signal(
                barrier, inc=1, device_id=device([sign * v for v in bits(octant)]), device_id_type=MESH
            )

    lane_head = lax.broadcasted_iota(jnp.int32, (T, T), 1) // (T // HEADS)
    sub = lax.broadcasted_iota(jnp.int32, (HEADS * WZ, 8, T), 1)

    level_base = where["lev"] * WZ

    def position_hot(shape, axis):
        group = lax.broadcasted_iota(jnp.int32, shape, axis) & (G - 1)
        source = lax.broadcasted_iota(jnp.int32, shape, 1 - axis)
        row = ((group >> 2) & 1) * YH + (group & 3)
        hit = (source == row * labels_ref.shape[1] + level_base + (group >> 3)) & ((group & 3) < YH)
        return hit.astype(jnp.float32).astype(jnp.bfloat16)

    cells = labels_ref.shape[0] * labels_ref.shape[1]
    label_cells = labels_ref[...].astype(jnp.float32).reshape(cells, labels_ref.shape[2]).astype(jnp.bfloat16)
    label_rows = jnp.dot(position_hot((G, cells), 0), label_cells, preferred_element_type=jnp.float32)
    by_lane = jnp.dot(position_hot((TABW, cells), 0), label_cells, preferred_element_type=jnp.float32)
    first = (lax.broadcasted_iota(jnp.int32, (G, labels_ref.shape[2]), 1) == 0).astype(jnp.float32)
    label_lanes = lax.dot_general(
        first.astype(jnp.bfloat16), by_lane.astype(jnp.bfloat16), (((1,), (1,)), ((), ())),
        preferred_element_type=jnp.float32,
    )
    regular = jnp.where((lax.broadcasted_iota(jnp.int32, (G, TABW), 1) & 3) < YH, 0.0, NEG)
    shifted = jnp.where(label_rows[:, :1] == label_lanes, regular, NEG)
    tabr[...] = jnp.zeros_like(tabr)

    def build_bias(b):
        raw = table_ref[b]
        total = None
        for zq in range(WZ):
            parts = []
            for a in range(WZ):
                for y in range(WY):
                    off = ((a * WZ + zq) * WY + y) * WY * SPAN
                    parts.append(raw[:, off : off + WY * SPAN])
            spread = jnp.dot(
                jnp.concatenate(parts, axis=0).astype(jnp.bfloat16), spread_ref[zq],
                preferred_element_type=jnp.float32,
            )
            total = spread if total is None else total + spread
        for a in range(WZ):
            for y in range(WY):
                row = (a * WY + y) * 8
                tabr[:, a * 8 + (y // YH) * 4 + y % YH, :] = total[row : row + HEADS]
        limit = shifted if b % 2 else regular
        table = jnp.where(limit[None] < 0.0, NEG, tabr[...]).reshape(HEADS * G, TABW)
        for c in range(2):
            for j in range(XH // 2):
                pair = []
                for xl in (2 * j, 2 * j + 1):
                    off = (WX - 1 - (c * XH + xl)) * G
                    rolled = pltpu.roll(table, (TABW - off) % TABW, axis=1)[:, :T]
                    pair.append(rolled.reshape(HEADS * WZ, 8, T))
                low = jnp.where(sub < 4, pair[0], pltpu.roll(pair[1], 4, axis=1))
                high = jnp.where(sub < 4, pltpu.roll(pair[0], 4, axis=1), pair[1])
                for h in range(HEADS):
                    for a in range(WZ):
                        row = h * T + (c * 4 + a * 2) * OROWS + j * 8
                        toep[row : row + 8, :] = low[h * WZ + a]
                        toep[row + OROWS : row + OROWS + 8, :] = high[h * WZ + a]
        bias[b] = jnp.dot(
            toep[...].astype(jnp.bfloat16), lanes_ref[...], preferred_element_type=jnp.float32
        )

    def layer_norm(values, gain_row):
        center = values - jnp.mean(values, axis=-1, keepdims=True)
        spread = jnp.mean(center * center, axis=-1, keepdims=True)
        return (center * lax.rsqrt(spread + 1e-05) * gain_row).astype(jnp.bfloat16)

    def block(b, stream):
        weight_copies[b * 4].wait()
        normed = layer_norm(stream, gains_ref[2 * b : 2 * b + 1, :])
        qkv = jnp.dot(normed, wq[b], preferred_element_type=jnp.float32).astype(jnp.bfloat16)
        width = T
        queries = qkv[:, :width]
        keys = qkv[:, width : 2 * width]
        values = qkv[:, 2 * width :]
        scale = (width // HEADS) ** (-0.5)
        total = None
        zero = jnp.zeros_like(queries)
        for h in range(HEADS):
            mine = lane_head == h
            scores = lax.dot_general(
                jnp.where(mine, queries, zero), keys, (((1,), (1,)), ((), ())),
                preferred_element_type=jnp.float32,
            )
            scores = scores * scale + bias[b, h * T : (h + 1) * T, :]
            terms = jnp.exp(scores - jnp.max(scores, axis=-1, keepdims=True))
            inverse = 1.0 / jnp.sum(terms, axis=-1, keepdims=True)
            weights = (terms * inverse).astype(jnp.bfloat16)
            part = jnp.dot(weights, jnp.where(mine, values, zero), preferred_element_type=jnp.float32)
            total = part if total is None else total + part
        weight_copies[b * 4 + 1].wait()
        attended = jnp.dot(total.astype(jnp.bfloat16), wo[b], preferred_element_type=jnp.float32)
        middle = (stream + attended.astype(jnp.bfloat16).astype(jnp.float32)).astype(jnp.bfloat16)
        middle = middle.astype(jnp.float32)
        normed_two = layer_norm(middle, gains_ref[2 * b + 1 : 2 * b + 2, :])
        weight_copies[b * 4 + 2].wait()
        up = jnp.dot(normed_two, wu[b], preferred_element_type=jnp.float32)
        hidden = (0.5 * up * (1.0 + lax.erf(up * 0.7071067811865476))).astype(jnp.bfloat16)
        weight_copies[b * 4 + 3].wait()
        down = lax.dot_general(
            hidden, wd[b], (((1,), (1,)), ((), ())), preferred_element_type=jnp.float32
        )
        return (middle + down).astype(jnp.bfloat16).astype(jnp.float32)

    def start_exchange(step, stream):
        send_buf[step] = stream.reshape(OCT, OROWS, T).astype(jnp.bfloat16)
        copies = []
        for octant in range(OCT):
            there = OCT - 1 - octant
            offsets = bits(octant) if step % 2 else [v - 1 for v in bits(octant)]
            if any(offsets):
                copy = pltpu.make_async_remote_copy(
                    src_ref=send_buf.at[step, octant],
                    dst_ref=recv_buf.at[step, there],
                    send_sem=send_sem.at[step, octant],
                    recv_sem=recv_sem.at[step, there],
                    device_id=device(offsets),
                    device_id_type=MESH,
                )
                copy.start()
                copies.append(copy)
            else:
                recv_buf[step, there] = stream[octant * OROWS : (octant + 1) * OROWS].astype(jnp.bfloat16)
        return copies

    def finish_exchange(step, copies):
        for copy in copies:
            copy.wait_recv()
        return recv_buf[step].astype(jnp.float32).reshape(T, T)

    grid_buf[...] = jnp.zeros_like(grid_buf)
    grid_buf[:, :WX, :] = fields_ref[...].astype(jnp.float32)
    rows = grid_buf[...].reshape(WZ * WY * 16, T).astype(jnp.bfloat16)
    constant_copies[0].wait()
    stream = jnp.dot(place_ref[...], rows, preferred_element_type=jnp.float32)
    constant_copies[1].wait()
    constant_copies[2].wait()
    build_bias(0)
    sent = []
    for b in range(BLOCKS):
        stream = block(b, stream)
        if b == 0:
            pl.semaphore_wait(barrier, 2 * (OCT - 1))
        copies = start_exchange(b, stream)
        sent += copies
        if b + 1 < BLOCKS:
            build_bias(b + 1)
        stream = finish_exchange(b, copies)
    constant_copies[3].wait()
    placed = jnp.dot(back_ref[...], stream.astype(jnp.bfloat16), preferred_element_type=jnp.float32)
    out_ref[...] = placed.reshape(WZ * WY, 16, T)[:, :WX, :].astype(jnp.bfloat16)
    for copy in sent:
        copy.wait_send()


def per_device(fields, w_qkv, w_out, w_up, w_down, gains, bias_table, labels):
    levels, lat_rows, lon_cols, width = fields.shape
    place_in, lanes, spread = token_maps()
    w_down = w_down.transpose(0, 2, 1)
    labels = labels.transpose(1, 0, 2)
    table = lax.dynamic_index_in_dim(bias_table[:, :, 0], lax.axis_index("lev"), 1, keepdims=False)
    table = jnp.pad(table.astype(jnp.float32), ((0, 0), (0, 8 - HEADS), (0, 0)))
    vmem = pl.BlockSpec(memory_space=pltpu.VMEM)
    hbm = pl.BlockSpec(memory_space=pltpu.HBM)
    out = pl.pallas_call(
        kernel,
        out_shape=jax.ShapeDtypeStruct((levels * lat_rows, lon_cols, width), jnp.bfloat16),
        in_specs=[vmem] * 4 + [hbm] * 8,
        out_specs=vmem,
        scratch_shapes=[
            pltpu.VMEM(place_in.shape, jnp.bfloat16),
            pltpu.VMEM(place_in.T.shape, jnp.bfloat16),
            pltpu.VMEM(lanes.shape, jnp.bfloat16),
            pltpu.VMEM(spread.shape, jnp.bfloat16),
            pltpu.VMEM(w_qkv.shape, jnp.bfloat16),
            pltpu.VMEM(w_out.shape, jnp.bfloat16),
            pltpu.VMEM(w_up.shape, jnp.bfloat16),
            pltpu.VMEM(w_down.shape, jnp.bfloat16),
            pltpu.VMEM((WZ * WY, 16, width), jnp.float32),
            pltpu.VMEM((HEADS, G, TABW), jnp.float32),
            pltpu.VMEM((HEADS * T, T), jnp.float32),
            pltpu.VMEM((BLOCKS, HEADS * T, T), jnp.float32),
            pltpu.VMEM((BLOCKS, OCT, OROWS, width), jnp.bfloat16),
            pltpu.VMEM((BLOCKS, OCT, OROWS, width), jnp.bfloat16),
            pltpu.SemaphoreType.DMA((4,)),
            pltpu.SemaphoreType.DMA((BLOCKS, 4)),
            pltpu.SemaphoreType.DMA((BLOCKS, OCT)),
            pltpu.SemaphoreType.DMA((BLOCKS, OCT)),
        ],
        compiler_params=pltpu.CompilerParams(
            collective_id=0, has_side_effects=True, vmem_limit_bytes=66_000_000
        ),
        name="earth_blocks",
    )(
        fields.reshape(levels * lat_rows, lon_cols, width),
        table,
        labels,
        gains.reshape(BLOCKS * 2, width),
        jnp.asarray(place_in, jnp.bfloat16),
        jnp.asarray(place_in.T, jnp.bfloat16),
        jnp.asarray(lanes, jnp.bfloat16),
        jnp.asarray(spread, jnp.bfloat16),
        w_qkv, w_out, w_up, w_down,
    )
    return out.reshape(fields.shape)


def solution(mesh):
    in_specs = (
        P("lev", "lat", "lon", None),
        P(),
        P(),
        P(),
        P(),
        P(),
        P(None, None, "lat", None, None),
        P(None, "lat", "lon"),
    )
    out_specs = P("lev", "lat", "lon", None)
    return jax.shard_map(
        per_device, mesh=mesh, in_specs=in_specs, out_specs=out_specs, check_vma=False
    )
```
